32 devices in a mesh: grp: 8 (over z, core), sub: 4 (over y, x).
Axes of the slice: x: 2, y: 2, z: 4, core: 2. Of those that a mesh axis runs over, the one named last changes fastest.
Arguments:
- coarse_op: float32 [256, 64, 576], P(('grp', 'sub'))
- right_side: float32 [256, 64, 64], P(('grp', 'sub')), may hold values from -6 to 6
- owner_map: int32 [256], replicated, may hold values from 0 to 255, as said below
- neighbor_table: int32 [256, 8], replicated, may hold values from 0 to 255, as said below
Outputs:
- solution: float32 [256, 64, 64], P(('grp', 'sub'))
The draws below stay inside these ranges and needn't reach their ends.
Inputs may be any that keep to these rules, and one draw needn't show every extreme that they name: `owner_map`: a permutation of 0 .. 255. `neighbor_table`: row t lists the neighbours of coarse site t on a periodic 4^4 lattice in the order +x, -x, +y, -y, +z, -z, +t, -t; lattice positions carry the site numbers in a permuted order.
All inputs are finite; a program needn't handle non-finite values.
Results may differ from the reference program's by a relative error of at most 0.0001.
Values sent between devices are 32-bit elements; how exact they have to be, the bound alone decides.
A program may use at most 64 MiB of HBM per device.

```python
import jax
import jax.numpy as jnp
from jax import lax

LAT = 4
DOF = 64
RHS = 64
ITERS = 3
HOPS = 8
SITES = 256


def draw_coarse_op(key, part):
    noise_key = jax.random.fold_in(key, 11)
    diag_key = jax.random.fold_in(key, 12)
    spread = 0.6 / (9.0 * DOF) ** 0.5
    noise = jax.random.normal(noise_key, (SITES, DOF, 9 * DOF), jnp.float32) * spread
    diag = jnp.exp(jax.random.uniform(diag_key, (SITES, DOF), jnp.float32, 0.0, 1.0986123))
    unit = jnp.eye(DOF, 9 * DOF, dtype=jnp.float32)
    return noise + diag[:, :, None] * unit[None]


def draw_owner_map(key, part):
    return jax.random.permutation(jax.random.fold_in(key, 21), SITES).astype(jnp.int32)


def draw_neighbor_table(key, part):
    relabel = jax.random.permutation(jax.random.fold_in(key, 31), SITES).astype(jnp.int32)
    position = jnp.arange(SITES, dtype=jnp.int32)
    columns = []
    for axis_dim in range(4):
        stride = LAT ** axis_dim
        coord = position // stride % LAT
        for offset in (1, -1):
            moved = position + ((coord + offset) % LAT - coord) * stride
            columns.append(relabel[moved])
    table = jnp.stack(columns, axis=1).astype(jnp.int32)
    return jnp.zeros((SITES, HOPS), jnp.int32).at[relabel].set(table)


def shard_levels(rng, dims, split, smallest, high):
    level, own = 1.0, jax.random.fold_in(rng, 6)
    for dim, shards_of in split:
        heights = jnp.exp(jax.random.uniform(jax.random.fold_in(own, dim), (shards_of,), jnp.float32, smallest / len(split), high / len(split)))
        level = level * jnp.repeat(heights, dims[dim] // shards_of).reshape([-1 if axis == dim else 1 for axis in range(len(dims))])
    return level


def gaussian(stream_key, dims, scale, limit, shards=(), held_as=jnp.bfloat16):
    array = scale * jax.random.normal(stream_key, dims, jnp.float32)
    if shards:
        array = array * shard_levels(stream_key, dims, shards, -0.22, 0.18)
    return jnp.clip(array, -limit, limit).astype(held_as)


def setup_inputs(seed: int = 0) -> dict:
    key_of = jax.random.split(jax.random.key(seed), 5)
    return {
        "coarse_op": draw_coarse_op(jax.random.fold_in(key_of[4], 71), 0),
        "right_side": gaussian(key_of[1], (SITES, DOF, RHS), 1.0, 6.0, ((0, 32),), jnp.float32),
        "owner_map": draw_owner_map(jax.random.fold_in(key_of[4], 71), 0),
        "neighbor_table": draw_neighbor_table(jax.random.fold_in(key_of[4], 71), 0),
    }


def inner_product(first, second):
    return lax.optimization_barrier(jnp.sum(first * second, axis=(0, 1)))

def reference(coarse_op, right_side, owner_map, neighbor_table):
    site_ids = jnp.arange(SITES, dtype=jnp.int32)
    inverse = lax.optimization_barrier(jnp.sum(jnp.where(owner_map[None, :] == site_ids[:, None], site_ids[None, :], 0), axis=1)).astype(jnp.int32)
    link = inverse[neighbor_table[owner_map]]

    def apply_op(vector):
        stacked = jnp.concatenate([vector[:, None], vector[link]], axis=1).reshape(SITES, 9 * DOF, RHS)
        return jnp.einsum('sac,scr->sar', coarse_op, stacked, precision=lax.Precision.HIGHEST)
    beta = jnp.sqrt(inner_product(right_side, right_side))
    krylov = [right_side / beta]
    hess = jnp.zeros((ITERS + 1, ITERS, RHS), jnp.float32)
    for column in range(ITERS):
        image = apply_op(krylov[column])
        coeffs = [inner_product(vector, image) for vector in krylov]
        for index_i in range(column + 1):
            image = image - coeffs[index_i] * krylov[index_i]
            hess = hess.at[index_i, column].set(coeffs[index_i])
        norm_value = jnp.sqrt(inner_product(image, image))
        hess = hess.at[column + 1, column].set(norm_value)
        krylov.append(image / norm_value)
    gram_matrix = jnp.einsum('ijr,ikr->rjk', hess, hess, precision=lax.Precision.HIGHEST)
    projected = (beta[None, :] * hess[0]).T
    weights = jnp.linalg.solve(gram_matrix, projected[..., None])[..., 0]
    solution = jnp.zeros_like(right_side)
    for column in range(ITERS):
        solution = solution + weights[:, column][None, None, :] * krylov[column]
    return solution
```

```python
import functools
import math

import jax
import jax.numpy as jnp
from jax import lax
from jax.experimental import pallas as pl
from jax.experimental.pallas import tpu as pltpu
from jax.sharding import PartitionSpec as P

LANES = 128
MESH = pl.DeviceIdType.MESH
F32 = jnp.float32
BF16 = jnp.bfloat16


def ring_order(count):
    side = math.isqrt(count)
    if side * side != count or side % 2:
        return list(range(count))
    order = list(range(side))
    for row in range(1, side):
        columns = range(side - 1, 0, -1) if row % 2 else range(1, side)
        order += [row * side + column for column in columns]
    return order + [row * side for row in range(side - 1, 0, -1)]


def lookup(table, index):
    found = jnp.int32(table[0])
    for place in range(1, len(table)):
        found = jnp.where(index == place, jnp.int32(table[place]), found)
    return found


def split(value):
    high = value.astype(BF16)
    return high, (value - high.astype(F32)).astype(BF16)


def kernel(
    planes, subs, per_dev, dof, half, hops,
    place_ref, table_ref, owner_ref, rhs_ref, op_ref, out_ref,
    vec0, vec1, vec2, image_ref, op_other, cp_high, cp_low, links, parts, sent, received,
    z_send, z_recv, r_send, r_recv, p_send, p_recv, s_send, s_recv, local_sem,
):
    pack = LANES // half
    rows = dof // pack
    block = 2 * per_dev
    chips = planes * subs
    sites = chips * block
    grp, sub = lax.axis_index("grp"), lax.axis_index("sub")
    plane, core = grp // 2, grp % 2
    partner = (plane * 2 + (1 - core), sub)
    me = plane * subs + sub
    order = ring_order(subs)
    where_in_ring = [order.index(s) for s in range(subs)]
    ring_pos = lookup(where_in_ring, sub)

    def ring_sub(offset):
        return lookup(order, lax.rem(ring_pos + offset + subs, subs))

    right, left = ring_sub(1), ring_sub(-1)

    def chip_device(chip):
        return (chip // subs * 2 + core, lax.rem(chip, subs))

    barrier = pltpu.get_barrier_semaphore()
    pl.semaphore_signal(barrier, inc=1, device_id=partner, device_id_type=MESH)

    @pl.loop(1, chips)
    def _(step):
        pl.semaphore_signal(
            barrier, inc=1, device_id=chip_device(lax.rem(me + step, chips)), device_id_type=MESH
        )

    pl.semaphore_wait(barrier, chips)

    def remote(src, dst, send, recv, device):
        return pltpu.make_async_remote_copy(
            src_ref=src, dst_ref=dst, send_sem=send, recv_sem=recv, device_id=device, device_id_type=MESH
        )

    own_rows = pl.ds(me * block + core * per_dev, per_dev)
    other_rows = pl.ds(me * block + (1 - core) * per_dev, per_dev)
    rhs_swap = remote(rhs_ref.at[1 - core], vec0.at[own_rows], p_send.at[0], p_recv.at[0], partner)
    rhs_swap.start()
    op_swap = remote(op_ref, op_other, p_send.at[1], p_recv.at[1], partner)
    op_swap.start()
    rhs_keep = pltpu.make_async_copy(rhs_ref.at[core], vec0.at[own_rows], local_sem)
    rhs_keep.start()
    rhs_keep.wait()
    rhs_swap.wait()

    full_steps = (subs - 1) // 2
    ring_steps = subs // 2
    keys = [(0, 0)] + [(way, dist) for dist in range(1, planes) for way in (0, 1)]

    def gather(number, vec, meanwhile=None):
        def at(chip_plane, chip_sub, piece=None):
            start = (chip_plane * subs + chip_sub) * block
            if piece is None:
                return vec.at[pl.ds(start, block)]
            return vec.at[pl.ds(start + piece * per_dev, per_dev)]

        def plane_of(key):
            way, dist = key
            return plane - dist if way == 0 else plane + dist

        def present(key):
            way, dist = key
            return plane >= dist if way == 0 else plane + dist < planes

        def guarded(key, action):
            if key[1] == 0:
                action()
            else:
                pl.when(present(key))(action)

        def z_copy(way, dist):
            src_plane = plane - (dist - 1) if way == 0 else plane + (dist - 1)
            next_plane = plane + 1 if way == 0 else plane - 1
            ref = at(src_plane, sub)
            return remote(
                ref, ref, z_send.at[number, way, dist], z_recv.at[number, way, dist],
                (next_plane * 2 + core, sub),
            )

        def z_goes(way):
            return plane < planes - 1 if way == 0 else plane > 0

        def z_arrival(key):
            way, dist = key
            ref = at(plane_of(key), sub)
            return remote(
                ref, ref, z_send.at[number, way, dist], z_recv.at[number, way, dist], (grp, sub)
            )

        def ring_copy(key, way, step, arriving):
            offset = step if arriving else step - 1
            src = ring_sub(-offset if way == 0 else offset)
            piece = way if 2 * step == subs else None
            ref = at(plane_of(key), src, piece)
            index = keys.index(key)
            return remote(
                ref, ref, r_send.at[number, index, way, step], r_recv.at[number, index, way, step],
                (grp, right if way == 0 else left),
            )

        def z_forward(way, dist):
            if dist < planes:
                pl.when(z_goes(way))(lambda: z_copy(way, dist).start())

        def ring_start(key, step):
            if step <= ring_steps:
                for way in (0, 1):
                    ring_copy(key, way, step, False).start()

        def ring_follow(key):
            for step in range(1, ring_steps):
                for way in (0, 1):
                    ring_copy(key, way, step, True).wait_recv()
                    ring_copy(key, way, step + 1, False).start()

        def ring_last(key):
            if ring_steps:
                for way in (0, 1):
                    ring_copy(key, way, ring_steps, True).wait_recv()

        def arrive(key):
            def action():
                z_arrival(key).wait_recv()
                z_forward(key[0], key[1] + 1)
                ring_start(key, 1)

            guarded(key, action)

        for way in (0, 1):
            z_forward(way, 1)
        ring_start((0, 0), 1)
        if meanwhile is not None:
            meanwhile[0]()
        behind = [(0, 0)]
        for dist in range(1, planes):
            now = [key for key in keys if key[1] == dist]
            for key in now:
                arrive(key)
            for key in behind:
                guarded(key, functools.partial(ring_follow, key))
            behind = now
            if meanwhile is not None and dist < len(meanwhile):
                meanwhile[dist]()
        for key in behind:
            guarded(key, functools.partial(ring_follow, key))
        for key in keys:
            guarded(key, functools.partial(ring_last, key))

        for dist in range(1, planes):
            for way in (0, 1):
                goes = jnp.logical_and(z_goes(way), present((way, dist - 1)))
                pl.when(goes)(lambda way=way, dist=dist: z_copy(way, dist).wait_send())

        def ring_sends(key):
            for step in range(1, ring_steps + 1):
                for way in (0, 1):
                    ring_copy(key, way, step, False).wait_send()

        for key in keys:
            guarded(key, functools.partial(ring_sends, key))

    width = (hops + 1) * dof
    depth = (hops + 1) * rows

    def regroup(source, first):
        high, low = split(source[...].reshape(per_dev * dof, width))
        at_row = lax.broadcasted_iota(jnp.int32, (width, depth), 0)
        at_column = lax.broadcasted_iota(jnp.int32, (width, depth), 1)
        for quarter in range(pack):
            wanted = at_column // rows * dof + quarter * rows + at_column % rows
            pick = jnp.where(at_row == wanted, 1.0, 0.0).astype(F32).astype(BF16)
            for value, kept in ((high, cp_high), (low, cp_low)):
                moved = jnp.dot(value, pick, preferred_element_type=F32).astype(BF16)
                kept[first : first + per_dev, quarter * dof : (quarter + 1) * dof, :] = moved.reshape(
                    per_dev, dof, depth
                )

    def find_links():
        @pl.loop(0, per_dev)
        def _(local):
            for side in (0, 1):
                slot_grp = plane * 2 + (core if side == 0 else 1 - core)
                slot = (slot_grp * subs + sub) * per_dev + local
                coarse = owner_ref[slot]
                for hop in range(hops):
                    links[(side * per_dev + local) * hops + hop] = place_ref[table_ref[coarse * hops + hop]]

    def prepare():
        find_links()
        regroup(op_ref, 0)

    def prepare_other():
        op_swap.wait()
        regroup(op_other, per_dev)

    lane_group = lax.broadcasted_iota(jnp.int32, (rows, LANES), 1) // half

    def apply_op(vec, over, store):
        def one(index, base, count_row):
            own = me * block + count_row
            pieces = [vec[own]] + [vec[links[index * hops + hop]] for hop in range(hops)]
            high, low = split(jnp.concatenate(pieces, axis=0))
            both = jnp.concatenate([high, low], axis=1)
            first = jnp.dot(cp_high[index], both, preferred_element_type=F32)
            second = jnp.dot(cp_low[index], high, preferred_element_type=F32)
            product = first[:, :LANES] + first[:, LANES:] + second
            total = None
            for turn in range(pack):
                picked = None
                for quarter in range(pack):
                    start = quarter * dof + (quarter + turn) % pack * rows
                    term = product[start : start + rows]
                    picked = term if picked is None else jnp.where(lane_group == quarter, term, picked)
                if turn:
                    picked = pltpu.roll(picked, turn * half, 1)
                total = picked if total is None else total + picked
            store(count_row, total / over)

        for side in (0, 1):
            base = (core if side == 0 else 1 - core) * per_dev

            @pl.loop(0, per_dev, unroll=min(4, per_dev))
            def _(local):
                one(side * per_dev + local, base, base + local)

    chunk = math.gcd(sites, 16)

    def sweep(body, count):
        def step(index, accs):
            return tuple(a + t for a, t in zip(accs, body(pl.ds(index * chunk, chunk))))

        accs = lax.fori_loop(0, sites // chunk, step, (jnp.zeros((rows, LANES), F32),) * count)
        return [fold(acc) for acc in accs]

    def fold(acc):
        total = jnp.sum(acc, axis=0, keepdims=True)
        total = jnp.broadcast_to(total, (rows, LANES))
        shift = half
        while shift < LANES:
            total = total + pltpu.roll(total, shift, 1)
            shift *= 2
        return total

    def dots(first, second):
        return jnp.sum(first * second, axis=0)

    def store_into(vec):
        def store(row, value):
            vec[me * block + row] = value

        return store

    gather(0, vec0, (prepare, prepare_other))
    (norm_sq,) = sweep(lambda s: (dots(vec0[s], vec0[s]),), 1)
    beta = jnp.sqrt(norm_sq)
    apply_op(vec0, beta, store_into(vec1))
    gather(1, vec1)
    (inner,) = sweep(lambda s: (dots(vec0[s], vec1[s]),), 1)
    h00 = inner / beta
    scale0 = h00 / beta

    def orthogonal1(s):
        left_over = vec1[s] - scale0 * vec0[s]
        vec1[s] = left_over
        return (dots(left_over, left_over),)

    (norm_sq,) = sweep(orthogonal1, 1)
    h10 = jnp.sqrt(norm_sq)

    apply_op(vec1, h10, store_into(vec2))
    gather(2, vec2)

    def inner2(s):
        image = vec2[s]
        return dots(vec0[s], image), dots(vec1[s], image)

    first, second = sweep(inner2, 2)
    h01, h11 = first / beta, second / h10
    scale0, scale1 = h01 / beta, h11 / h10

    def orthogonal2(s):
        left_over = vec2[s] - scale0 * vec0[s] - scale1 * vec1[s]
        vec2[s] = left_over
        return (dots(left_over, left_over),)

    (norm_sq,) = sweep(orthogonal2, 1)
    h21 = jnp.sqrt(norm_sq)

    def store_image(row, value):
        image_ref[row] = value

    apply_op(vec2, h21, store_image)
    mine = pl.ds(me * block, block)
    image = image_ref[...]
    for place, vec in enumerate((vec0, vec1, vec2)):
        parts[me, place * rows : (place + 1) * rows] = dots(vec[mine], image)
    parts[me, 3 * rows : 4 * rows] = dots(image, image)

    def part_copy(step, arriving):
        chip = lax.rem(me - step + chips, chips) if arriving else me
        ref = parts.at[chip]
        return remote(
            ref, ref, s_send.at[step], s_recv.at[step], chip_device(lax.rem(me + step, chips))
        )

    @pl.loop(1, chips)
    def _(step):
        part_copy(step, False).start()

    @pl.loop(1, chips)
    def _(step):
        part_copy(step, True).wait_recv()

    @pl.loop(1, chips)
    def _(step):
        part_copy(step, False).wait_send()

    summed = jnp.sum(parts[...], axis=0)
    sums = [fold(summed[place * rows : (place + 1) * rows]) for place in range(4)]
    h02, h12, h22 = sums[0] / beta, sums[1] / h10, sums[2] / h21

    g00 = h00 * h00 + h10 * h10
    g01 = h00 * h01 + h10 * h11
    g02 = h00 * h02 + h10 * h12
    g11 = h01 * h01 + h11 * h11 + h21 * h21
    g12 = h01 * h02 + h11 * h12 + h21 * h22
    g22 = sums[3]
    l00 = jnp.sqrt(g00)
    l10, l20 = g01 / l00, g02 / l00
    l11 = jnp.sqrt(g11 - l10 * l10)
    l21 = (g12 - l20 * l10) / l11
    l22 = jnp.sqrt(g22 - l20 * l20 - l21 * l21)
    t0 = beta * h00 / l00
    t1 = (beta * h01 - l10 * t0) / l11
    t2 = (beta * h02 - l20 * t0 - l21 * t1) / l22
    y2 = t2 / l22
    y1 = (t1 - l21 * y2) / l11
    y0 = (t0 - l10 * y1 - l20 * y2) / l00
    y0, y1, y2 = y0 / beta, y1 / h10, y2 / h21

    sent[...] = y0 * vec0[other_rows] + y1 * vec1[other_rows] + y2 * vec2[other_rows]
    swap = remote(sent, received, p_send.at[2], p_recv.at[2], partner)
    swap.start()
    out_ref[core] = y0 * vec0[own_rows] + y1 * vec1[own_rows] + y2 * vec2[own_rows]
    swap.wait()
    out_ref[1 - core] = received[...]


def per_device(coarse_op, right_side, owner_map, neighbor_table):
    subs, planes = lax.axis_size("sub"), lax.axis_size("grp") // 2
    per_dev, dof, width = coarse_op.shape
    rhs = right_side.shape[2]
    hops = width // dof - 1
    half = rhs // 2
    pack = LANES // half
    rows = dof // pack
    site_count = owner_map.shape[0]
    block = 2 * per_dev
    depth = (hops + 1) * rows

    slots = jnp.arange(site_count, dtype=jnp.int32)
    owner_block = slots // per_dev
    slot_grp, slot_sub = owner_block // subs, owner_block % subs
    place = ((slot_grp // 2 * subs + slot_sub) * 2 + slot_grp % 2) * per_dev + slots % per_dev
    place_of = jnp.sum(jnp.where(owner_map[None, :] == slots[:, None], place[None, :], 0), axis=1)

    packed = right_side.reshape(per_dev, pack, rows, 2, half).transpose(3, 0, 2, 1, 4)
    packed = packed.reshape(2, per_dev, rows, LANES)
    smem = pl.BlockSpec(memory_space=pltpu.SMEM)
    vmem = pl.BlockSpec(memory_space=pltpu.VMEM)
    keys = 2 * planes - 1
    dma = pltpu.SemaphoreType.DMA
    vector = pltpu.VMEM((site_count, rows, LANES), F32)
    small = pltpu.VMEM((per_dev, rows, LANES), F32)
    solved = pl.pallas_call(
        functools.partial(kernel, planes, subs, per_dev, dof, half, hops),
        out_shape=jax.ShapeDtypeStruct((2, per_dev, rows, LANES), F32),
        in_specs=[smem, smem, smem, vmem, vmem],
        out_specs=vmem,
        scratch_shapes=[
            vector,
            vector,
            vector,
            pltpu.VMEM((block, rows, LANES), F32),
            pltpu.VMEM((per_dev, dof, width), F32),
            pltpu.VMEM((block, pack * dof, depth), BF16),
            pltpu.VMEM((block, pack * dof, depth), BF16),
            pltpu.SMEM((block * hops,), jnp.int32),
            pltpu.VMEM((planes * subs, 4 * rows, LANES), F32),
            small,
            small,
            dma((3, 2, planes)),
            dma((3, 2, planes)),
            dma((3, keys, 2, subs // 2 + 1)),
            dma((3, keys, 2, subs // 2 + 1)),
            dma((3,)),
            dma((3,)),
            dma((planes * subs,)),
            dma((planes * subs,)),
            dma,
        ],
        compiler_params=pltpu.CompilerParams(
            collective_id=0, has_side_effects=True, vmem_limit_bytes=48 * 1024 * 1024
        ),
    )(place_of, neighbor_table.reshape(-1), owner_map, packed, coarse_op)
    solved = solved.reshape(2, per_dev, rows, pack, half).transpose(1, 3, 2, 0, 4)
    return solved.reshape(per_dev, dof, rhs)


def solution(mesh):
    placed = (P(("grp", "sub"), None, None), P(("grp", "sub"), None, None), P(), P())
    return jax.shard_map(
        per_device,
        mesh=mesh,
        in_specs=placed,
        out_specs=P(("grp", "sub"), None, None),
        check_vma=False,
    )
```

```python
import functools
import math

import jax
import jax.numpy as jnp
from jax import lax
from jax.experimental import pallas as pl
from jax.experimental.pallas import tpu as pltpu
from jax.sharding import PartitionSpec as P

LANES = 128
MESH = pl.DeviceIdType.MESH
F32 = jnp.float32
BF16 = jnp.bfloat16


def ring_order(count):
    side = math.isqrt(count)
    if side * side != count or side % 2:
        return list(range(count))
    order = list(range(side))
    for row in range(1, side):
        columns = range(side - 1, 0, -1) if row % 2 else range(1, side)
        order += [row * side + column for column in columns]
    return order + [row * side for row in range(side - 1, 0, -1)]


def lookup(table, index):
    found = jnp.int32(table[0])
    for place in range(1, len(table)):
        found = jnp.where(index == place, jnp.int32(table[place]), found)
    return found


def split(value):
    high = value.astype(BF16)
    return high, (value - high.astype(F32)).astype(BF16)


def kernel(
    planes, subs, per_dev, dof, half, hops,
    place_ref, table_ref, owner_ref, rhs_ref, op_hbm, out_ref,
    packed, vec0, vec1, vec2, image_ref, op_ref, op_other, cp_high, cp_low, links, parts, sent, received,
    z_send, z_recv, r_send, r_recv, p_send, p_recv, s_send, s_recv, local_sem, load_sem,
):
    pack = LANES // half
    rows = dof // pack
    block = 2 * per_dev
    chips = planes * subs
    sites = chips * block
    grp, sub = lax.axis_index("grp"), lax.axis_index("sub")
    plane, core = grp // 2, grp % 2
    partner = (plane * 2 + (1 - core), sub)
    me = plane * subs + sub
    order = ring_order(subs)
    where_in_ring = [order.index(s) for s in range(subs)]
    ring_pos = lookup(where_in_ring, sub)

    def ring_sub(offset):
        return lookup(order, lax.rem(ring_pos + offset + subs, subs))

    right, left = ring_sub(1), ring_sub(-1)

    def chip_device(chip):
        return (chip // subs * 2 + core, lax.rem(chip, subs))

    op_load = pltpu.make_async_copy(op_hbm, op_ref, load_sem)
    op_load.start()
    barrier = pltpu.get_barrier_semaphore()

    def greet(device):
        pl.semaphore_signal(barrier, inc=1, device_id=device, device_id_type=MESH)

    greet(partner)
    if subs > 1:
        greet((grp, right))
        greet((grp, left))
    pl.when(plane > 0)(lambda: greet(((plane - 1) * 2 + core, sub)))
    pl.when(plane < planes - 1)(lambda: greet(((plane + 1) * 2 + core, sub)))
    for side in (0, 1):
        columns = [
            rhs_ref[:, quarter * rows : (quarter + 1) * rows, side * half : (side + 1) * half]
            for quarter in range(pack)
        ]
        packed[side] = jnp.concatenate(columns, axis=2)
    ends = jnp.where(plane > 0, 1, 0) + jnp.where(plane < planes - 1, 1, 0)
    pl.semaphore_wait(barrier, (3 if subs > 1 else 1) + ends)

    def remote(src, dst, send, recv, device):
        return pltpu.make_async_remote_copy(
            src_ref=src, dst_ref=dst, send_sem=send, recv_sem=recv, device_id=device, device_id_type=MESH
        )

    own_rows = pl.ds(me * block + core * per_dev, per_dev)
    other_rows = pl.ds(me * block + (1 - core) * per_dev, per_dev)
    rhs_swap = remote(packed.at[1 - core], vec0.at[own_rows], p_send.at[0], p_recv.at[0], partner)
    rhs_swap.start()
    op_swap = remote(op_ref, op_other, p_send.at[1], p_recv.at[1], partner)
    rhs_keep = pltpu.make_async_copy(packed.at[core], vec0.at[own_rows], local_sem)
    rhs_keep.start()
    rhs_keep.wait()
    rhs_swap.wait()

    ring_steps = subs // 2
    keys = [(0, 0)] + [(way, dist) for dist in range(1, planes) for way in (0, 1)]
    opposite = ring_sub(ring_steps)
    reach = planes // 2 if ring_steps and subs % 2 == 0 else 0

    def gather(number, vec, meanwhile=()):
        def at(chip_plane, chip_sub, piece=None):
            start = (chip_plane * subs + chip_sub) * block
            if piece is None:
                return vec.at[pl.ds(start, block)]
            return vec.at[pl.ds(start + piece * per_dev, per_dev)]

        def plane_of(way, dist):
            return plane - dist if way == 0 else plane + dist

        def present(way, dist):
            return plane >= dist if way == 0 else plane + dist < planes

        def guarded(key, action, *more):
            if key[1] == 0:
                action(key, *more)
            else:
                pl.when(present(*key))(lambda: action(key, *more))

        def keys_at(dist):
            return [key for key in keys if key[1] == dist]

        def z_copy(stream, way, dist, arriving):
            ref = at(plane_of(way, dist if arriving else dist - 1), opposite if stream else sub)
            next_plane = plane + 1 if way == 0 else plane - 1
            return remote(
                ref, ref, z_send.at[number, stream, way, dist], z_recv.at[number, stream, way, dist],
                (next_plane * 2 + core, sub),
            )

        def z_goes(way):
            return plane < planes - 1 if way == 0 else plane > 0

        def z_forward(stream, way, dist):
            if dist <= (reach if stream else planes - 1):
                pl.when(z_goes(way))(lambda: z_copy(stream, way, dist, False).start())

        def z_arrive(key, stream):
            z_copy(stream, *key, True).wait_recv()
            z_forward(stream, key[0], key[1] + 1)

        def steps_of(key):
            return ring_steps - 1 if 1 <= key[1] <= reach else ring_steps

        def ring_copy(key, way, step, arriving):
            offset = step if arriving else step - 1
            src = ring_sub(-offset if way == 0 else offset)
            piece = way if 2 * step == subs else None
            ref = at(plane_of(*key), src, piece)
            index = keys.index(key)
            return remote(
                ref, ref, r_send.at[number, index, way, step], r_recv.at[number, index, way, step],
                (grp, right if way == 0 else left),
            )

        def ring_start(key):
            if steps_of(key):
                for way in (0, 1):
                    ring_copy(key, way, 1, False).start()

        def ring_follow(key):
            for step in range(1, steps_of(key)):
                for way in (0, 1):
                    ring_copy(key, way, step, True).wait_recv()
                    ring_copy(key, way, step + 1, False).start()

        def ring_last(key):
            if steps_of(key):
                for way in (0, 1):
                    ring_copy(key, way, steps_of(key), True).wait_recv()

        def ring_sends(key):
            for step in range(1, steps_of(key) + 1):
                for way in (0, 1):
                    ring_copy(key, way, step, False).wait_send()

        own = (0, 0)
        for way in (0, 1):
            z_forward(0, way, 1)
        ring_start(own)
        for task in meanwhile[:1]:
            task()
        if planes == 1:
            ring_follow(own)
            ring_last(own)
        across = list(range(1, reach + 1))
        for dist in range(1, planes):
            for key in keys_at(dist):
                guarded(key, z_arrive, 0)
            if dist == 1:
                ring_follow(own)
            for key in keys_at(dist):
                guarded(key, ring_start)
            for key in keys_at(dist - 1) if dist > 1 else ():
                guarded(key, ring_follow)
            if dist == min(2, planes - 1):
                ring_last(own)
                for way in (0, 1):
                    z_forward(1, way, 1)
            elif dist > 2 and across:
                for key in keys_at(across.pop(0)):
                    guarded(key, z_arrive, 1)
            for task in meanwhile[dist : dist + 1]:
                task()
        for key in keys_at(planes - 1) if planes > 1 else ():
            guarded(key, ring_follow)
        for dist in across:
            for key in keys_at(dist):
                guarded(key, z_arrive, 1)
        for key in keys[1:]:
            guarded(key, ring_last)

        def z_sends(stream, way, dist):
            goes = jnp.logical_and(z_goes(way), present(way, dist - 1))
            pl.when(goes)(lambda: z_copy(stream, way, dist, False).wait_send())

        for stream in (0, 1):
            for dist in range(1, reach + 1 if stream else planes):
                for way in (0, 1):
                    z_sends(stream, way, dist)
        for key in keys:
            guarded(key, ring_sends)

    width = (hops + 1) * dof
    depth = (hops + 1) * rows

    def regroup(source, first):
        high, low = split(source[...].reshape(per_dev * dof, width))
        at_row = lax.broadcasted_iota(jnp.int32, (width, depth), 0)
        at_column = lax.broadcasted_iota(jnp.int32, (width, depth), 1)
        for quarter in range(pack):
            wanted = at_column // rows * dof + quarter * rows + at_column % rows
            pick = jnp.where(at_row == wanted, 1.0, 0.0).astype(F32).astype(BF16)
            for value, kept in ((high, cp_high), (low, cp_low)):
                moved = jnp.dot(value, pick, preferred_element_type=F32).astype(BF16)
                kept[first : first + per_dev, quarter * dof : (quarter + 1) * dof, :] = moved.reshape(
                    per_dev, dof, depth
                )

    def find_links():
        @pl.loop(0, per_dev)
        def _(local):
            for side in (0, 1):
                slot_grp = plane * 2 + (core if side == 0 else 1 - core)
                slot = (slot_grp * subs + sub) * per_dev + local
                coarse = owner_ref[slot]
                for hop in range(hops):
                    links[(side * per_dev + local) * hops + hop] = place_ref[table_ref[hop, coarse]]

    def prepare():
        op_load.wait()
        op_swap.start()
        find_links()
        regroup(op_ref, 0)

    def prepare_other():
        op_swap.wait()
        regroup(op_other, per_dev)

    lane_group = lax.broadcasted_iota(jnp.int32, (rows, LANES), 1) // half

    def apply_op(vec, over, store):
        def one(index, base, count_row):
            own = me * block + count_row
            pieces = [vec[own]] + [vec[links[index * hops + hop]] for hop in range(hops)]
            high, low = split(jnp.concatenate(pieces, axis=0))
            both = jnp.concatenate([high, low], axis=1)
            first = jnp.dot(cp_high[index], both, preferred_element_type=F32)
            second = jnp.dot(cp_low[index], high, preferred_element_type=F32)
            product = first[:, :LANES] + first[:, LANES:] + second
            total = None
            for turn in range(pack):
                picked = None
                for quarter in range(pack):
                    start = quarter * dof + (quarter + turn) % pack * rows
                    term = product[start : start + rows]
                    picked = term if picked is None else jnp.where(lane_group == quarter, term, picked)
                if turn:
                    picked = pltpu.roll(picked, turn * half, 1)
                total = picked if total is None else total + picked
            store(count_row, total / over)

        for side in (0, 1):
            base = (core if side == 0 else 1 - core) * per_dev

            @pl.loop(0, per_dev, unroll=min(4, per_dev))
            def _(local):
                one(side * per_dev + local, base, base + local)

    chunk = math.gcd(sites, 16)

    def sweep(body, count):
        def step(index, accs):
            return tuple(a + t for a, t in zip(accs, body(pl.ds(index * chunk, chunk))))

        accs = lax.fori_loop(0, sites // chunk, step, (jnp.zeros((rows, LANES), F32),) * count)
        return [fold(acc) for acc in accs]

    def fold(acc):
        total = jnp.sum(acc, axis=0, keepdims=True)
        total = jnp.broadcast_to(total, (rows, LANES))
        shift = half
        while shift < LANES:
            total = total + pltpu.roll(total, shift, 1)
            shift *= 2
        return total

    def dots(first, second):
        return jnp.sum(first * second, axis=0)

    def store_into(vec):
        def store(row, value):
            vec[me * block + row] = value

        return store

    gather(0, vec0, (prepare, prepare_other))
    (norm_sq,) = sweep(lambda s: (dots(vec0[s], vec0[s]),), 1)
    beta = jnp.sqrt(norm_sq)
    apply_op(vec0, beta, store_into(vec1))
    gather(1, vec1)
    (inner,) = sweep(lambda s: (dots(vec0[s], vec1[s]),), 1)
    h00 = inner / beta
    scale0 = h00 / beta

    def orthogonal1(s):
        left_over = vec1[s] - scale0 * vec0[s]
        vec1[s] = left_over
        return (dots(left_over, left_over),)

    (norm_sq,) = sweep(orthogonal1, 1)
    h10 = jnp.sqrt(norm_sq)

    apply_op(vec1, h10, store_into(vec2))
    gather(2, vec2)

    def inner2(s):
        image = vec2[s]
        return dots(vec0[s], image), dots(vec1[s], image)

    first, second = sweep(inner2, 2)
    h01, h11 = first / beta, second / h10
    scale0, scale1 = h01 / beta, h11 / h10

    def orthogonal2(s):
        left_over = vec2[s] - scale0 * vec0[s] - scale1 * vec1[s]
        vec2[s] = left_over
        return (dots(left_over, left_over),)

    (norm_sq,) = sweep(orthogonal2, 1)
    h21 = jnp.sqrt(norm_sq)

    def store_image(row, value):
        image_ref[row] = value

    apply_op(vec2, h21, store_image)
    mine = pl.ds(me * block, block)
    image = image_ref[...]
    products = [dots(vec[mine], image) for vec in (vec0, vec1, vec2)] + [dots(image, image)]
    at_row = lax.broadcasted_iota(jnp.int32, (8, LANES), 0)
    part = jnp.zeros((8, LANES), F32)
    for place, product in enumerate(products):
        part = jnp.where(at_row == place, jnp.sum(product, axis=0, keepdims=True), part)
    parts[me] = part

    def part_copy(step, arriving):
        chip = lax.rem(me - step + chips, chips) if arriving else me
        ref = parts.at[chip]
        return remote(
            ref, ref, s_send.at[step], s_recv.at[step], chip_device(lax.rem(me + step, chips))
        )

    @pl.loop(1, chips)
    def _(step):
        part_copy(step, False).start()

    @pl.loop(1, chips)
    def _(step):
        part_copy(step, True).wait_recv()

    @pl.loop(1, chips)
    def _(step):
        part_copy(step, False).wait_send()

    summed = jnp.sum(parts[...], axis=0)
    sums = [fold(summed[place : place + 1]) for place in range(4)]
    h02, h12, h22 = sums[0] / beta, sums[1] / h10, sums[2] / h21

    g00 = h00 * h00 + h10 * h10
    g01 = h00 * h01 + h10 * h11
    g02 = h00 * h02 + h10 * h12
    g11 = h01 * h01 + h11 * h11 + h21 * h21
    g12 = h01 * h02 + h11 * h12 + h21 * h22
    g22 = sums[3]
    l00 = jnp.sqrt(g00)
    l10, l20 = g01 / l00, g02 / l00
    l11 = jnp.sqrt(g11 - l10 * l10)
    l21 = (g12 - l20 * l10) / l11
    l22 = jnp.sqrt(g22 - l20 * l20 - l21 * l21)
    t0 = beta * h00 / l00
    t1 = (beta * h01 - l10 * t0) / l11
    t2 = (beta * h02 - l20 * t0 - l21 * t1) / l22
    y2 = t2 / l22
    y1 = (t1 - l21 * y2) / l11
    y0 = (t0 - l10 * y1 - l20 * y2) / l00
    y0, y1, y2 = y0 / beta, y1 / h10, y2 / h21

    sent[...] = y0 * vec0[other_rows] + y1 * vec1[other_rows] + y2 * vec2[other_rows]
    swap = remote(sent, received, p_send.at[2], p_recv.at[2], partner)
    swap.start()
    kept = y0 * vec0[own_rows] + y1 * vec1[own_rows] + y2 * vec2[own_rows]
    swap.wait()
    came = received[...]
    first = jnp.where(core == 0, kept, came)
    second = jnp.where(core == 0, came, kept)
    for quarter in range(pack):
        lanes = slice(quarter * half, (quarter + 1) * half)
        out_ref[:, quarter * rows : (quarter + 1) * rows, :] = jnp.concatenate(
            [first[:, :, lanes], second[:, :, lanes]], axis=2
        )


def per_device(coarse_op, right_side, owner_map, neighbor_table):
    subs, planes = lax.axis_size("sub"), lax.axis_size("grp") // 2
    per_dev, dof, width = coarse_op.shape
    rhs = right_side.shape[2]
    hops = width // dof - 1
    half = rhs // 2
    pack = LANES // half
    rows = dof // pack
    site_count = owner_map.shape[0]
    block = 2 * per_dev
    depth = (hops + 1) * rows

    slots = jnp.arange(site_count, dtype=jnp.int32)
    owner_block = slots // per_dev
    slot_grp, slot_sub = owner_block // subs, owner_block % subs
    place = ((slot_grp // 2 * subs + slot_sub) * 2 + slot_grp % 2) * per_dev + slots % per_dev
    place_of = jnp.sum(jnp.where(owner_map[None, :] == slots[:, None], place[None, :], 0), axis=1)

    smem = pl.BlockSpec(memory_space=pltpu.SMEM)
    vmem = pl.BlockSpec(memory_space=pltpu.VMEM)
    keys = 2 * planes - 1
    dma = pltpu.SemaphoreType.DMA
    vector = pltpu.VMEM((site_count, rows, LANES), F32)
    small = pltpu.VMEM((per_dev, rows, LANES), F32)
    return pl.pallas_call(
        functools.partial(kernel, planes, subs, per_dev, dof, half, hops),
        out_shape=jax.ShapeDtypeStruct(right_side.shape, F32),
        in_specs=[smem, smem, smem, vmem, pl.BlockSpec(memory_space=pl.ANY)],
        out_specs=vmem,
        scratch_shapes=[
            pltpu.VMEM((2, per_dev, rows, LANES), F32),
            vector,
            vector,
            vector,
            pltpu.VMEM((block, rows, LANES), F32),
            pltpu.VMEM((per_dev, dof, width), F32),
            pltpu.VMEM((per_dev, dof, width), F32),
            pltpu.VMEM((block, pack * dof, depth), BF16),
            pltpu.VMEM((block, pack * dof, depth), BF16),
            pltpu.SMEM((block * hops,), jnp.int32),
            pltpu.VMEM((planes * subs, 8, LANES), F32),
            small,
            small,
            dma((3, 2, 2, planes)),
            dma((3, 2, 2, planes)),
            dma((3, keys, 2, subs // 2 + 1)),
            dma((3, keys, 2, subs // 2 + 1)),
            dma((3,)),
            dma((3,)),
            dma((planes * subs,)),
            dma((planes * subs,)),
            dma,
            dma,
        ],
        compiler_params=pltpu.CompilerParams(
            collective_id=0, has_side_effects=True, vmem_limit_bytes=48 * 1024 * 1024
        ),
    )(place_of, neighbor_table.T, owner_map, right_side, coarse_op)


def solution(mesh):
    placed = (P(("grp", "sub"), None, None), P(("grp", "sub"), None, None), P(), P())
    return jax.shard_map(
        per_device,
        mesh=mesh,
        in_specs=placed,
        out_specs=P(("grp", "sub"), None, None),
        check_vma=False,
    )
```

```python
import functools
import math

import jax
import jax.numpy as jnp
from jax import lax
from jax.experimental import pallas as pl
from jax.experimental.pallas import tpu as pltpu
from jax.sharding import PartitionSpec as P

LANES = 128
MESH = pl.DeviceIdType.MESH
F32 = jnp.float32
BF16 = jnp.bfloat16


def ring_order(count):
    side = math.isqrt(count)
    if side * side != count or side % 2:
        return list(range(count))
    order = list(range(side))
    for row in range(1, side):
        columns = range(side - 1, 0, -1) if row % 2 else range(1, side)
        order += [row * side + column for column in columns]
    return order + [row * side for row in range(side - 1, 0, -1)]


def lookup(table, index):
    found = jnp.int32(table[0])
    for place in range(1, len(table)):
        found = jnp.where(index == place, jnp.int32(table[place]), found)
    return found


def split(value):
    high = value.astype(BF16)
    return high, (value - high.astype(F32)).astype(BF16)


def kernel(
    planes, subs, per_dev, dof, half, hops,
    place_ref, table_ref, owner_ref, rhs_ref, op_hbm, out_ref,
    packed, vec0, vec1, vec2, image_ref, op_ref, op_other, cp_high, cp_low, links, parts, sent, received,
    z_send, z_recv, r_send, r_recv, p_send, p_recv, s_send, s_recv, local_sem, load_sem,
):
    pack = LANES // half
    rows = dof // pack
    block = 2 * per_dev
    chips = planes * subs
    sites = chips * block
    grp, sub = lax.axis_index("grp"), lax.axis_index("sub")
    plane, core = grp // 2, grp % 2
    partner = (plane * 2 + (1 - core), sub)
    me = plane * subs + sub
    order = ring_order(subs)
    where_in_ring = [order.index(s) for s in range(subs)]
    ring_pos = lookup(where_in_ring, sub)

    def ring_sub(offset):
        return lookup(order, lax.rem(ring_pos + offset + subs, subs))

    right, left = ring_sub(1), ring_sub(-1)

    def chip_device(chip):
        return (chip // subs * 2 + core, lax.rem(chip, subs))

    op_load = pltpu.make_async_copy(op_hbm, op_ref, load_sem)
    op_load.start()
    barrier = pltpu.get_barrier_semaphore()

    def greet(device):
        pl.semaphore_signal(barrier, inc=1, device_id=device, device_id_type=MESH)

    greet(partner)
    if subs > 1:
        greet((grp, right))
        greet((grp, left))
    pl.when(plane > 0)(lambda: greet(((plane - 1) * 2 + core, sub)))
    pl.when(plane < planes - 1)(lambda: greet(((plane + 1) * 2 + core, sub)))
    for side in (0, 1):
        columns = [
            rhs_ref[:, quarter * rows : (quarter + 1) * rows, side * half : (side + 1) * half]
            for quarter in range(pack)
        ]
        packed[side] = jnp.concatenate(columns, axis=2)
    ends = jnp.where(plane > 0, 1, 0) + jnp.where(plane < planes - 1, 1, 0)
    pl.semaphore_wait(barrier, (3 if subs > 1 else 1) + ends)

    def remote(src, dst, send, recv, device):
        return pltpu.make_async_remote_copy(
            src_ref=src, dst_ref=dst, send_sem=send, recv_sem=recv, device_id=device, device_id_type=MESH
        )

    own_rows = pl.ds(me * block + core * per_dev, per_dev)
    other_rows = pl.ds(me * block + (1 - core) * per_dev, per_dev)
    rhs_swap = remote(packed.at[1 - core], vec0.at[own_rows], p_send.at[0], p_recv.at[0], partner)
    rhs_swap.start()
    op_swap = remote(op_ref, op_other, p_send.at[1], p_recv.at[1], partner)
    rhs_keep = pltpu.make_async_copy(packed.at[core], vec0.at[own_rows], local_sem)
    rhs_keep.start()

    ring_steps = subs // 2
    keys = [(0, 0)] + [(way, dist) for dist in range(1, planes) for way in (0, 1)]
    opposite = ring_sub(ring_steps)
    reach = (planes - 1) // 2 if ring_steps and subs % 2 == 0 else 0

    halves = (0, 1)
    ways = (0, 1)

    def gathering(number, vec):
        def at(chip_plane, chip_sub, piece):
            first = core if piece == 0 else 1 - core
            return vec.at[pl.ds((chip_plane * subs + chip_sub) * block + first * per_dev, per_dev)]

        def plane_of(way, dist):
            return plane - dist if way == 0 else plane + dist

        def present(way, dist):
            return plane >= dist if way == 0 else plane + dist < planes

        def guarded(key, action, *more):
            if key[1] == 0:
                action(key, *more)
            else:
                pl.when(present(*key))(lambda: action(key, *more))

        def keys_at(dist):
            return [key for key in keys if key[1] == dist]

        def z_copy(stream, way, dist, piece, arriving):
            ref = at(plane_of(way, dist if arriving else dist - 1), opposite if stream else sub, piece)
            next_plane = plane + 1 if way == 0 else plane - 1
            index = (number, stream, way, dist - 1, piece)
            return remote(ref, ref, z_send.at[index], z_recv.at[index], (next_plane * 2 + core, sub))

        def z_goes(way):
            return plane < planes - 1 if way == 0 else plane > 0

        def z_forward(stream, way, dist, piece):
            if dist <= (reach if stream else planes - 1):
                pl.when(z_goes(way))(lambda: z_copy(stream, way, dist, piece, False).start())

        def z_arrive(key, stream, piece):
            z_copy(stream, *key, piece, True).wait_recv()
            z_forward(stream, key[0], key[1] + 1, piece)

        def ring_moves(key):
            steps = ring_steps - 1 if 1 <= key[1] <= reach else ring_steps
            return [
                [(way, piece) for way in ways for piece in (way, 1 - way) if 2 * step != subs or piece == way]
                for step in range(1, steps + 1)
            ]

        def ring_copy(key, step, way, piece, arriving):
            offset = step if arriving else step - 1
            ref = at(plane_of(*key), ring_sub(-offset if way == 0 else offset), piece)
            index = (number, keys.index(key), way, step - 1, piece)
            return remote(
                ref, ref, r_send.at[index], r_recv.at[index], (grp, right if way == 0 else left)
            )

        def ring_start(key, pieces=halves):
            for way, piece in (ring_moves(key) or [[]])[0]:
                if piece in pieces:
                    ring_copy(key, 1, way, piece, False).start()

        def ring_follow(key):
            moves = ring_moves(key)
            for step in range(2, len(moves) + 1):
                for way, piece in moves[step - 1]:
                    ring_copy(key, step - 1, way, piece, True).wait_recv()
                    ring_copy(key, step, way, piece, False).start()

        def ring_last(key):
            moves = ring_moves(key)
            for step in range(1, len(moves) + 1):
                for way, piece in moves[step - 1]:
                    if step == len(moves) or (way, piece) not in moves[step]:
                        ring_copy(key, step, way, piece, True).wait_recv()

        def ring_sends(key):
            for step, moves in enumerate(ring_moves(key)):
                for way, piece in moves:
                    ring_copy(key, step + 1, way, piece, False).wait_send()

        own = (0, 0)

        def begin(piece):
            for way in ways:
                z_forward(0, way, 1, piece)
            ring_start(own, (piece,))

        def finish(meanwhile=()):
            for task in meanwhile[:1]:
                task()
            if planes == 1:
                ring_follow(own)
                ring_last(own)
            across = list(range(1, reach + 1))
            for dist in range(1, planes):
                for piece in halves:
                    for key in keys_at(dist):
                        guarded(key, z_arrive, 0, piece)
                    if dist == 1 and piece == 0:
                        ring_follow(own)
                for key in keys_at(dist):
                    guarded(key, ring_start)
                for key in keys_at(dist - 1) if dist > 1 else ():
                    guarded(key, ring_follow)
                if dist == min(2, planes - 1):
                    ring_last(own)
                    for piece in halves:
                        for way in ways:
                            z_forward(1, way, 1, piece)
                elif dist > 2 and across:
                    pair = across.pop(0)
                    for piece in halves:
                        for key in keys_at(pair):
                            guarded(key, z_arrive, 1, piece)
                for task in meanwhile[dist : dist + 1]:
                    task()
            for key in keys_at(planes - 1) if planes > 1 else ():
                guarded(key, ring_follow)
            for dist in across:
                for piece in halves:
                    for key in keys_at(dist):
                        guarded(key, z_arrive, 1, piece)
            for key in keys[1:]:
                guarded(key, ring_last)

            def z_sends(stream, way, dist, piece):
                goes = jnp.logical_and(z_goes(way), present(way, dist - 1))
                pl.when(goes)(lambda: z_copy(stream, way, dist, piece, False).wait_send())

            for stream in (0, 1):
                for dist in range(1, reach + 1 if stream else planes):
                    for way in ways:
                        for piece in halves:
                            z_sends(stream, way, dist, piece)
            for key in keys:
                guarded(key, ring_sends)

        return begin, finish

    width = (hops + 1) * dof
    depth = (hops + 1) * rows

    def regroup(source, first):
        high, low = split(source[...].reshape(per_dev * dof, width))
        at_row = lax.broadcasted_iota(jnp.int32, (width, depth), 0)
        at_column = lax.broadcasted_iota(jnp.int32, (width, depth), 1)
        for quarter in range(pack):
            wanted = at_column // rows * dof + quarter * rows + at_column % rows
            pick = jnp.where(at_row == wanted, 1.0, 0.0).astype(F32).astype(BF16)
            for value, kept in ((high, cp_high), (low, cp_low)):
                moved = jnp.dot(value, pick, preferred_element_type=F32).astype(BF16)
                kept[first : first + per_dev, quarter * dof : (quarter + 1) * dof, :] = moved.reshape(
                    per_dev, dof, depth
                )

    def find_links():
        @pl.loop(0, per_dev)
        def _(local):
            for side in (0, 1):
                slot_grp = plane * 2 + (core if side == 0 else 1 - core)
                slot = (slot_grp * subs + sub) * per_dev + local
                coarse = owner_ref[slot]
                for hop in range(hops):
                    links[(side * per_dev + local) * hops + hop] = place_ref[table_ref[hop, coarse]]

    def prepare():
        op_load.wait()
        op_swap.start()
        find_links()
        regroup(op_ref, 0)

    def prepare_other():
        op_swap.wait()
        regroup(op_other, per_dev)

    lane_group = lax.broadcasted_iota(jnp.int32, (rows, LANES), 1) // half

    def apply_op(vec, over, store, then=None):
        def one(index, count_row):
            own = me * block + count_row
            pieces = [vec[own]] + [vec[links[index * hops + hop]] for hop in range(hops)]
            high, low = split(jnp.concatenate(pieces, axis=0))
            both = jnp.concatenate([high, low], axis=1)
            first = jnp.dot(cp_high[index], both, preferred_element_type=F32)
            second = jnp.dot(cp_low[index], high, preferred_element_type=F32)
            product = first[:, :LANES] + first[:, LANES:] + second
            total = None
            for turn in range(pack):
                picked = None
                for quarter in range(pack):
                    start = quarter * dof + (quarter + turn) % pack * rows
                    term = product[start : start + rows]
                    picked = term if picked is None else jnp.where(lane_group == quarter, term, picked)
                if turn:
                    picked = pltpu.roll(picked, turn * half, 1)
                total = picked if total is None else total + picked
            store(count_row, total / over)

        for side in (0, 1):
            base = (core if side == 0 else 1 - core) * per_dev

            @pl.loop(0, per_dev, unroll=min(4, per_dev))
            def _(local):
                one(side * per_dev + local, base + local)

            if then is not None:
                then(side)

    chunk = math.gcd(sites, 16)

    def sweep(body, count):
        def step(index, accs):
            return tuple(a + t for a, t in zip(accs, body(pl.ds(index * chunk, chunk))))

        accs = lax.fori_loop(0, sites // chunk, step, (jnp.zeros((rows, LANES), F32),) * count)
        return [fold(acc) for acc in accs]

    def fold(acc):
        total = jnp.sum(acc, axis=0, keepdims=True)
        total = jnp.broadcast_to(total, (rows, LANES))
        shift = half
        while shift < LANES:
            total = total + pltpu.roll(total, shift, 1)
            shift *= 2
        return total

    def dots(first, second):
        return jnp.sum(first * second, axis=0)

    def store_into(vec):
        def store(row, value):
            vec[me * block + row] = value

        return store

    begin, finish = gathering(0, vec0)
    rhs_keep.wait()
    begin(0)
    rhs_swap.wait()
    begin(1)
    finish((prepare, prepare_other))
    (norm_sq,) = sweep(lambda s: (dots(vec0[s], vec0[s]),), 1)
    beta = jnp.sqrt(norm_sq)
    begin, finish = gathering(1, vec1)
    apply_op(vec0, beta, store_into(vec1), begin)
    finish()
    (inner,) = sweep(lambda s: (dots(vec0[s], vec1[s]),), 1)
    h00 = inner / beta
    scale0 = h00 / beta

    def orthogonal1(s):
        left_over = vec1[s] - scale0 * vec0[s]
        vec1[s] = left_over
        return (dots(left_over, left_over),)

    (norm_sq,) = sweep(orthogonal1, 1)
    h10 = jnp.sqrt(norm_sq)

    begin, finish = gathering(2, vec2)
    apply_op(vec1, h10, store_into(vec2), begin)
    finish()

    def inner2(s):
        image = vec2[s]
        return dots(vec0[s], image), dots(vec1[s], image)

    first, second = sweep(inner2, 2)
    h01, h11 = first / beta, second / h10
    scale0, scale1 = h01 / beta, h11 / h10

    def orthogonal2(s):
        left_over = vec2[s] - scale0 * vec0[s] - scale1 * vec1[s]
        vec2[s] = left_over
        return (dots(left_over, left_over),)

    (norm_sq,) = sweep(orthogonal2, 1)
    h21 = jnp.sqrt(norm_sq)

    def store_image(row, value):
        image_ref[row] = value

    apply_op(vec2, h21, store_image)
    mine = pl.ds(me * block, block)
    image = image_ref[...]
    products = [dots(vec[mine], image) for vec in (vec0, vec1, vec2)] + [dots(image, image)]
    at_row = lax.broadcasted_iota(jnp.int32, (8, LANES), 0)
    part = jnp.zeros((8, LANES), F32)
    for place, product in enumerate(products):
        part = jnp.where(at_row == place, jnp.sum(product, axis=0, keepdims=True), part)
    parts[me] = part

    def part_copy(step, arriving):
        chip = lax.rem(me - step + chips, chips) if arriving else me
        ref = parts.at[chip]
        return remote(
            ref, ref, s_send.at[step], s_recv.at[step], chip_device(lax.rem(me + step, chips))
        )

    @pl.loop(1, chips)
    def _(step):
        part_copy(step, False).start()

    @pl.loop(1, chips)
    def _(step):
        part_copy(step, True).wait_recv()

    @pl.loop(1, chips)
    def _(step):
        part_copy(step, False).wait_send()

    summed = jnp.sum(parts[...], axis=0)
    sums = [fold(summed[place : place + 1]) for place in range(4)]
    h02, h12, h22 = sums[0] / beta, sums[1] / h10, sums[2] / h21

    g00 = h00 * h00 + h10 * h10
    g01 = h00 * h01 + h10 * h11
    g02 = h00 * h02 + h10 * h12
    g11 = h01 * h01 + h11 * h11 + h21 * h21
    g12 = h01 * h02 + h11 * h12 + h21 * h22
    g22 = sums[3]
    l00 = jnp.sqrt(g00)
    l10, l20 = g01 / l00, g02 / l00
    l11 = jnp.sqrt(g11 - l10 * l10)
    l21 = (g12 - l20 * l10) / l11
    l22 = jnp.sqrt(g22 - l20 * l20 - l21 * l21)
    t0 = beta * h00 / l00
    t1 = (beta * h01 - l10 * t0) / l11
    t2 = (beta * h02 - l20 * t0 - l21 * t1) / l22
    y2 = t2 / l22
    y1 = (t1 - l21 * y2) / l11
    y0 = (t0 - l10 * y1 - l20 * y2) / l00
    y0, y1, y2 = y0 / beta, y1 / h10, y2 / h21

    sent[...] = y0 * vec0[other_rows] + y1 * vec1[other_rows] + y2 * vec2[other_rows]
    swap = remote(sent, received, p_send.at[2], p_recv.at[2], partner)
    swap.start()
    kept = y0 * vec0[own_rows] + y1 * vec1[own_rows] + y2 * vec2[own_rows]
    swap.wait()
    came = received[...]
    first = jnp.where(core == 0, kept, came)
    second = jnp.where(core == 0, came, kept)
    for quarter in range(pack):
        lanes = slice(quarter * half, (quarter + 1) * half)
        out_ref[:, quarter * rows : (quarter + 1) * rows, :] = jnp.concatenate(
            [first[:, :, lanes], second[:, :, lanes]], axis=2
        )


def per_device(coarse_op, right_side, owner_map, neighbor_table):
    subs, planes = lax.axis_size("sub"), lax.axis_size("grp") // 2
    per_dev, dof, width = coarse_op.shape
    rhs = right_side.shape[2]
    hops = width // dof - 1
    half = rhs // 2
    pack = LANES // half
    rows = dof // pack
    site_count = owner_map.shape[0]
    block = 2 * per_dev
    depth = (hops + 1) * rows

    slots = jnp.arange(site_count, dtype=jnp.int32)
    owner_block = slots // per_dev
    slot_grp, slot_sub = owner_block // subs, owner_block % subs
    place = ((slot_grp // 2 * subs + slot_sub) * 2 + slot_grp % 2) * per_dev + slots % per_dev
    place_of = jnp.sum(jnp.where(owner_map[None, :] == slots[:, None], place[None, :], 0), axis=1)

    smem = pl.BlockSpec(memory_space=pltpu.SMEM)
    vmem = pl.BlockSpec(memory_space=pltpu.VMEM)
    keys = 2 * planes - 1
    dma = pltpu.SemaphoreType.DMA
    vector = pltpu.VMEM((site_count, rows, LANES), F32)
    small = pltpu.VMEM((per_dev, rows, LANES), F32)
    return pl.pallas_call(
        functools.partial(kernel, planes, subs, per_dev, dof, half, hops),
        out_shape=jax.ShapeDtypeStruct(right_side.shape, F32),
        in_specs=[smem, smem, smem, vmem, pl.BlockSpec(memory_space=pl.ANY)],
        out_specs=vmem,
        scratch_shapes=[
            pltpu.VMEM((2, per_dev, rows, LANES), F32),
            vector,
            vector,
            vector,
            pltpu.VMEM((block, rows, LANES), F32),
            pltpu.VMEM((per_dev, dof, width), F32),
            pltpu.VMEM((per_dev, dof, width), F32),
            pltpu.VMEM((block, pack * dof, depth), BF16),
            pltpu.VMEM((block, pack * dof, depth), BF16),
            pltpu.SMEM((block * hops,), jnp.int32),
            pltpu.VMEM((planes * subs, 8, LANES), F32),
            small,
            small,
            dma((3, 2, 2, max(planes - 1, 1), 2)),
            dma((3, 2, 2, max(planes - 1, 1), 2)),
            dma((3, keys, 2, max(subs // 2, 1), 2)),
            dma((3, keys, 2, max(subs // 2, 1), 2)),
            dma((3,)),
            dma((3,)),
            dma((planes * subs,)),
            dma((planes * subs,)),
            dma,
            dma,
        ],
        compiler_params=pltpu.CompilerParams(
            collective_id=0, has_side_effects=True, vmem_limit_bytes=48 * 1024 * 1024
        ),
    )(place_of, neighbor_table.T, owner_map, right_side, coarse_op)


def solution(mesh):
    placed = (P(("grp", "sub"), None, None), P(("grp", "sub"), None, None), P(), P())
    return jax.shard_map(
        per_device,
        mesh=mesh,
        in_specs=placed,
        out_specs=P(("grp", "sub"), None, None),
        check_vma=False,
    )
```

```python
import functools
import math

import jax
import jax.numpy as jnp
from jax import lax
from jax.experimental import pallas as pl
from jax.experimental.pallas import tpu as pltpu
from jax.sharding import PartitionSpec as P

LANES = 128
MESH = pl.DeviceIdType.MESH
F32 = jnp.float32
BF16 = jnp.bfloat16


def ring_order(count):
    side = math.isqrt(count)
    if side * side != count or side % 2:
        return list(range(count))
    order = list(range(side))
    for row in range(1, side):
        columns = range(side - 1, 0, -1) if row % 2 else range(1, side)
        order += [row * side + column for column in columns]
    return order + [row * side for row in range(side - 1, 0, -1)]


def lookup(table, index):
    found = jnp.int32(table[0])
    for place in range(1, len(table)):
        found = jnp.where(index == place, jnp.int32(table[place]), found)
    return found


def split(value):
    high = value.astype(BF16)
    return high, (value - high.astype(F32)).astype(BF16)


def kernel(
    planes, subs, per_dev, dof, half, hops,
    place_ref, table_hbm, owner_hbm, rhs_hbm, op_hbm, out_ref,
    table_ref, owner_ref, rhs_ref, packed, vec0, vec1, vec2, image_ref, op_ref, op_other, cp_high, cp_low, links, parts, sent, received,
    z_send, z_recv, r_send, r_recv, p_send, p_recv, s_send, s_recv, local_sem, load_sem,
):
    pack = LANES // half
    rows = dof // pack
    block = 2 * per_dev
    chips = planes * subs
    sites = chips * block
    grp, sub = lax.axis_index("grp"), lax.axis_index("sub")
    plane, core = grp // 2, grp % 2
    partner = (plane * 2 + (1 - core), sub)
    me = plane * subs + sub
    order = ring_order(subs)
    where_in_ring = [order.index(s) for s in range(subs)]
    ring_pos = lookup(where_in_ring, sub)

    def ring_sub(offset):
        return lookup(order, lax.rem(ring_pos + offset + subs, subs))

    right, left = ring_sub(1), ring_sub(-1)

    def chip_device(chip):
        return (chip // subs * 2 + core, lax.rem(chip, subs))

    def load(source, kept, place):
        copy = pltpu.make_async_copy(source, kept, load_sem.at[place])
        copy.start()
        return copy

    rhs_load = load(rhs_hbm, rhs_ref, 0)
    op_load = load(op_hbm, op_ref, 1)
    table_load = load(table_hbm, table_ref, 2)
    owner_load = load(owner_hbm, owner_ref, 3)
    barrier = pltpu.get_barrier_semaphore()

    def greet(device):
        pl.semaphore_signal(barrier, inc=1, device_id=device, device_id_type=MESH)

    greet(partner)
    if subs > 1:
        greet((grp, right))
        greet((grp, left))
    pl.when(plane > 0)(lambda: greet(((plane - 1) * 2 + core, sub)))
    pl.when(plane < planes - 1)(lambda: greet(((plane + 1) * 2 + core, sub)))
    rhs_load.wait()
    for side in (0, 1):
        columns = [
            rhs_ref[:, quarter * rows : (quarter + 1) * rows, side * half : (side + 1) * half]
            for quarter in range(pack)
        ]
        packed[side] = jnp.concatenate(columns, axis=2)
    ends = jnp.where(plane > 0, 1, 0) + jnp.where(plane < planes - 1, 1, 0)
    pl.semaphore_wait(barrier, (3 if subs > 1 else 1) + ends)

    def remote(src, dst, send, recv, device):
        return pltpu.make_async_remote_copy(
            src_ref=src, dst_ref=dst, send_sem=send, recv_sem=recv, device_id=device, device_id_type=MESH
        )

    own_rows = pl.ds(me * block + core * per_dev, per_dev)
    other_rows = pl.ds(me * block + (1 - core) * per_dev, per_dev)
    rhs_swap = remote(packed.at[1 - core], vec0.at[own_rows], p_send.at[0], p_recv.at[0], partner)
    rhs_swap.start()
    op_swap = remote(op_ref, op_other, p_send.at[1], p_recv.at[1], partner)
    rhs_keep = pltpu.make_async_copy(packed.at[core], vec0.at[own_rows], local_sem)
    rhs_keep.start()

    ring_steps = subs // 2
    keys = [(0, 0)] + [(way, dist) for dist in range(1, planes) for way in (0, 1)]
    opposite = ring_sub(ring_steps)
    reach = (planes - 1) // 2 if ring_steps and subs % 2 == 0 else 0

    halves = (0, 1)
    ways = (0, 1)

    def gathering(number, vec):
        def at(chip_plane, chip_sub, piece):
            first = core if piece == 0 else 1 - core
            return vec.at[pl.ds((chip_plane * subs + chip_sub) * block + first * per_dev, per_dev)]

        def plane_of(way, dist):
            return plane - dist if way == 0 else plane + dist

        def present(way, dist):
            return plane >= dist if way == 0 else plane + dist < planes

        def guarded(key, action, *more):
            if key[1] == 0:
                action(key, *more)
            else:
                pl.when(present(*key))(lambda: action(key, *more))

        def keys_at(dist):
            return [key for key in keys if key[1] == dist]

        def z_copy(stream, way, dist, piece, arriving):
            ref = at(plane_of(way, dist if arriving else dist - 1), opposite if stream else sub, piece)
            next_plane = plane + 1 if way == 0 else plane - 1
            index = (number, stream, way, dist - 1, piece)
            return remote(ref, ref, z_send.at[index], z_recv.at[index], (next_plane * 2 + core, sub))

        def z_goes(way):
            return plane < planes - 1 if way == 0 else plane > 0

        def z_forward(stream, way, dist, piece):
            if dist <= (reach if stream else planes - 1):
                pl.when(z_goes(way))(lambda: z_copy(stream, way, dist, piece, False).start())

        def z_arrive(key, stream, piece):
            z_copy(stream, *key, piece, True).wait_recv()
            z_forward(stream, key[0], key[1] + 1, piece)

        def ring_moves(key):
            steps = ring_steps - 1 if 1 <= key[1] <= reach else ring_steps
            return [
                [(way, piece) for way in ways for piece in (way, 1 - way) if 2 * step != subs or piece == way]
                for step in range(1, steps + 1)
            ]

        def ring_copy(key, step, way, piece, arriving):
            offset = step if arriving else step - 1
            ref = at(plane_of(*key), ring_sub(-offset if way == 0 else offset), piece)
            index = (number, keys.index(key), way, step - 1, piece)
            return remote(
                ref, ref, r_send.at[index], r_recv.at[index], (grp, right if way == 0 else left)
            )

        def ring_start(key, pieces=halves):
            for way, piece in (ring_moves(key) or [[]])[0]:
                if piece in pieces:
                    ring_copy(key, 1, way, piece, False).start()

        def ring_follow(key):
            moves = ring_moves(key)
            for step in range(2, len(moves) + 1):
                for way, piece in moves[step - 1]:
                    ring_copy(key, step - 1, way, piece, True).wait_recv()
                    ring_copy(key, step, way, piece, False).start()

        def ring_last(key):
            moves = ring_moves(key)
            for step in range(1, len(moves) + 1):
                for way, piece in moves[step - 1]:
                    if step == len(moves) or (way, piece) not in moves[step]:
                        ring_copy(key, step, way, piece, True).wait_recv()

        def ring_sends(key):
            for step, moves in enumerate(ring_moves(key)):
                for way, piece in moves:
                    ring_copy(key, step + 1, way, piece, False).wait_send()

        own = (0, 0)

        def begin(piece):
            for way in ways:
                z_forward(0, way, 1, piece)
            ring_start(own, (piece,))

        def finish(meanwhile=()):
            for task in meanwhile[:1]:
                task()
            if planes == 1:
                ring_follow(own)
                ring_last(own)
            across = list(range(1, reach + 1))
            for dist in range(1, planes):
                for piece in halves:
                    for key in keys_at(dist):
                        guarded(key, z_arrive, 0, piece)
                    if dist == 1 and piece == 0:
                        ring_follow(own)
                for key in keys_at(dist):
                    guarded(key, ring_start)
                for key in keys_at(dist - 1) if dist > 1 else ():
                    guarded(key, ring_follow)
                if dist == min(2, planes - 1):
                    ring_last(own)
                    for piece in halves:
                        for way in ways:
                            z_forward(1, way, 1, piece)
                elif dist > 2 and across:
                    pair = across.pop(0)
                    for piece in halves:
                        for key in keys_at(pair):
                            guarded(key, z_arrive, 1, piece)
                for task in meanwhile[dist : dist + 1]:
                    task()
            for key in keys_at(planes - 1) if planes > 1 else ():
                guarded(key, ring_follow)
            for dist in across:
                for piece in halves:
                    for key in keys_at(dist):
                        guarded(key, z_arrive, 1, piece)
            for key in keys[1:]:
                guarded(key, ring_last)

            def z_sends(stream, way, dist, piece):
                goes = jnp.logical_and(z_goes(way), present(way, dist - 1))
                pl.when(goes)(lambda: z_copy(stream, way, dist, piece, False).wait_send())

            for stream in (0, 1):
                for dist in range(1, reach + 1 if stream else planes):
                    for way in ways:
                        for piece in halves:
                            z_sends(stream, way, dist, piece)
            for key in keys:
                guarded(key, ring_sends)

        return begin, finish

    width = (hops + 1) * dof
    depth = (hops + 1) * rows

    def regroup(source, first):
        high, low = split(source[...].reshape(per_dev * dof, width))
        at_row = lax.broadcasted_iota(jnp.int32, (width, depth), 0)
        at_column = lax.broadcasted_iota(jnp.int32, (width, depth), 1)
        for quarter in range(pack):
            wanted = at_column // rows * dof + quarter * rows + at_column % rows
            pick = jnp.where(at_row == wanted, 1.0, 0.0).astype(F32).astype(BF16)
            for value, kept in ((high, cp_high), (low, cp_low)):
                moved = jnp.dot(value, pick, preferred_element_type=F32).astype(BF16)
                kept[first : first + per_dev, quarter * dof : (quarter + 1) * dof, :] = moved.reshape(
                    per_dev, dof, depth
                )

    def find_links():
        table_load.wait()
        owner_load.wait()

        @pl.loop(0, per_dev)
        def _(local):
            for side in (0, 1):
                slot_grp = plane * 2 + (core if side == 0 else 1 - core)
                slot = (slot_grp * subs + sub) * per_dev + local
                coarse = owner_ref[slot]
                for hop in range(hops):
                    links[(side * per_dev + local) * hops + hop] = place_ref[table_ref[hop, coarse]]

    def prepare():
        op_load.wait()
        op_swap.start()
        find_links()
        regroup(op_ref, 0)

    def prepare_other():
        op_swap.wait()
        regroup(op_other, per_dev)

    lane_group = lax.broadcasted_iota(jnp.int32, (rows, LANES), 1) // half

    def apply_op(vec, over, store, then=None):
        def one(index, count_row):
            own = me * block + count_row
            pieces = [vec[own]] + [vec[links[index * hops + hop]] for hop in range(hops)]
            high, low = split(jnp.concatenate(pieces, axis=0))
            both = jnp.concatenate([high, low], axis=1)
            first = jnp.dot(cp_high[index], both, preferred_element_type=F32)
            second = jnp.dot(cp_low[index], high, preferred_element_type=F32)
            product = first[:, :LANES] + first[:, LANES:] + second
            total = None
            for turn in range(pack):
                picked = None
                for quarter in range(pack):
                    start = quarter * dof + (quarter + turn) % pack * rows
                    term = product[start : start + rows]
                    picked = term if picked is None else jnp.where(lane_group == quarter, term, picked)
                if turn:
                    picked = pltpu.roll(picked, turn * half, 1)
                total = picked if total is None else total + picked
            store(count_row, total / over)

        for side in (0, 1):
            base = (core if side == 0 else 1 - core) * per_dev

            @pl.loop(0, per_dev, unroll=min(4, per_dev))
            def _(local):
                one(side * per_dev + local, base + local)

            if then is not None:
                then(side)

    chunk = math.gcd(sites, 16)

    def sweep(body, count):
        def step(index, accs):
            return tuple(a + t for a, t in zip(accs, body(pl.ds(index * chunk, chunk))))

        accs = lax.fori_loop(0, sites // chunk, step, (jnp.zeros((rows, LANES), F32),) * count)
        return [fold(acc) for acc in accs]

    def fold(acc):
        total = jnp.sum(acc, axis=0, keepdims=True)
        total = jnp.broadcast_to(total, (rows, LANES))
        shift = half
        while shift < LANES:
            total = total + pltpu.roll(total, shift, 1)
            shift *= 2
        return total

    def dots(first, second):
        return jnp.sum(first * second, axis=0)

    def store_into(vec):
        def store(row, value):
            vec[me * block + row] = value

        return store

    begin, finish = gathering(0, vec0)
    rhs_keep.wait()
    begin(0)
    rhs_swap.wait()
    begin(1)
    finish((prepare, prepare_other))
    (norm_sq,) = sweep(lambda s: (dots(vec0[s], vec0[s]),), 1)
    beta = jnp.sqrt(norm_sq)
    begin, finish = gathering(1, vec1)
    apply_op(vec0, beta, store_into(vec1), begin)
    finish()
    (inner,) = sweep(lambda s: (dots(vec0[s], vec1[s]),), 1)
    h00 = inner / beta
    scale0 = h00 / beta

    def orthogonal1(s):
        left_over = vec1[s] - scale0 * vec0[s]
        vec1[s] = left_over
        return (dots(left_over, left_over),)

    (norm_sq,) = sweep(orthogonal1, 1)
    h10 = jnp.sqrt(norm_sq)

    begin, finish = gathering(2, vec2)
    apply_op(vec1, h10, store_into(vec2), begin)
    finish()

    def inner2(s):
        image = vec2[s]
        return dots(vec0[s], image), dots(vec1[s], image)

    first, second = sweep(inner2, 2)
    h01, h11 = first / beta, second / h10
    scale0, scale1 = h01 / beta, h11 / h10

    def orthogonal2(s):
        left_over = vec2[s] - scale0 * vec0[s] - scale1 * vec1[s]
        vec2[s] = left_over
        return (dots(left_over, left_over),)

    (norm_sq,) = sweep(orthogonal2, 1)
    h21 = jnp.sqrt(norm_sq)

    def store_image(row, value):
        image_ref[row] = value

    apply_op(vec2, h21, store_image)
    mine = pl.ds(me * block, block)
    image = image_ref[...]
    products = [dots(vec[mine], image) for vec in (vec0, vec1, vec2)] + [dots(image, image)]
    at_row = lax.broadcasted_iota(jnp.int32, (8, LANES), 0)
    part = jnp.zeros((8, LANES), F32)
    for place, product in enumerate(products):
        part = jnp.where(at_row == place, jnp.sum(product, axis=0, keepdims=True), part)
    parts[me] = part

    def part_copy(step, arriving):
        chip = lax.rem(me - step + chips, chips) if arriving else me
        ref = parts.at[chip]
        return remote(
            ref, ref, s_send.at[step], s_recv.at[step], chip_device(lax.rem(me + step, chips))
        )

    @pl.loop(1, chips)
    def _(step):
        part_copy(step, False).start()

    @pl.loop(1, chips)
    def _(step):
        part_copy(step, True).wait_recv()

    @pl.loop(1, chips)
    def _(step):
        part_copy(step, False).wait_send()

    summed = jnp.sum(parts[...], axis=0)
    sums = [fold(summed[place : place + 1]) for place in range(4)]
    h02, h12, h22 = sums[0] / beta, sums[1] / h10, sums[2] / h21

    g00 = h00 * h00 + h10 * h10
    g01 = h00 * h01 + h10 * h11
    g02 = h00 * h02 + h10 * h12
    g11 = h01 * h01 + h11 * h11 + h21 * h21
    g12 = h01 * h02 + h11 * h12 + h21 * h22
    g22 = sums[3]
    l00 = jnp.sqrt(g00)
    l10, l20 = g01 / l00, g02 / l00
    l11 = jnp.sqrt(g11 - l10 * l10)
    l21 = (g12 - l20 * l10) / l11
    l22 = jnp.sqrt(g22 - l20 * l20 - l21 * l21)
    t0 = beta * h00 / l00
    t1 = (beta * h01 - l10 * t0) / l11
    t2 = (beta * h02 - l20 * t0 - l21 * t1) / l22
    y2 = t2 / l22
    y1 = (t1 - l21 * y2) / l11
    y0 = (t0 - l10 * y1 - l20 * y2) / l00
    y0, y1, y2 = y0 / beta, y1 / h10, y2 / h21

    sent[...] = y0 * vec0[other_rows] + y1 * vec1[other_rows] + y2 * vec2[other_rows]
    swap = remote(sent, received, p_send.at[2], p_recv.at[2], partner)
    swap.start()
    kept = y0 * vec0[own_rows] + y1 * vec1[own_rows] + y2 * vec2[own_rows]
    swap.wait()
    came = received[...]
    first = jnp.where(core == 0, kept, came)
    second = jnp.where(core == 0, came, kept)
    for quarter in range(pack):
        lanes = slice(quarter * half, (quarter + 1) * half)
        out_ref[:, quarter * rows : (quarter + 1) * rows, :] = jnp.concatenate(
            [first[:, :, lanes], second[:, :, lanes]], axis=2
        )


def per_device(coarse_op, right_side, owner_map, neighbor_table):
    subs, planes = lax.axis_size("sub"), lax.axis_size("grp") // 2
    per_dev, dof, width = coarse_op.shape
    rhs = right_side.shape[2]
    hops = width // dof - 1
    half = rhs // 2
    pack = LANES // half
    rows = dof // pack
    site_count = owner_map.shape[0]
    block = 2 * per_dev
    depth = (hops + 1) * rows

    slots = jnp.arange(site_count, dtype=jnp.int32)
    owner_block = slots // per_dev
    slot_grp, slot_sub = owner_block // subs, owner_block % subs
    place = ((slot_grp // 2 * subs + slot_sub) * 2 + slot_grp % 2) * per_dev + slots % per_dev
    place_of = jnp.sum(jnp.where(owner_map[None, :] == slots[:, None], place[None, :], 0), axis=1)

    smem = pl.BlockSpec(memory_space=pltpu.SMEM)
    vmem = pl.BlockSpec(memory_space=pltpu.VMEM)
    keys = 2 * planes - 1
    dma = pltpu.SemaphoreType.DMA
    vector = pltpu.VMEM((site_count, rows, LANES), F32)
    small = pltpu.VMEM((per_dev, rows, LANES), F32)
    return pl.pallas_call(
        functools.partial(kernel, planes, subs, per_dev, dof, half, hops),
        out_shape=jax.ShapeDtypeStruct(right_side.shape, F32),
        in_specs=[smem] + [pl.BlockSpec(memory_space=pltpu.HBM)] * 4,
        out_specs=vmem,
        scratch_shapes=[
            pltpu.SMEM((hops, site_count), jnp.int32),
            pltpu.SMEM((site_count,), jnp.int32),
            pltpu.VMEM(right_side.shape, F32),
            pltpu.VMEM((2, per_dev, rows, LANES), F32),
            vector,
            vector,
            vector,
            pltpu.VMEM((block, rows, LANES), F32),
            pltpu.VMEM((per_dev, dof, width), F32),
            pltpu.VMEM((per_dev, dof, width), F32),
            pltpu.VMEM((block, pack * dof, depth), BF16),
            pltpu.VMEM((block, pack * dof, depth), BF16),
            pltpu.SMEM((block * hops,), jnp.int32),
            pltpu.VMEM((planes * subs, 8, LANES), F32),
            small,
            small,
            dma((3, 2, 2, max(planes - 1, 1), 2)),
            dma((3, 2, 2, max(planes - 1, 1), 2)),
            dma((3, keys, 2, max(subs // 2, 1), 2)),
            dma((3, keys, 2, max(subs // 2, 1), 2)),
            dma((3,)),
            dma((3,)),
            dma((planes * subs,)),
            dma((planes * subs,)),
            dma,
            dma((4,)),
        ],
        compiler_params=pltpu.CompilerParams(
            collective_id=0, has_side_effects=True, vmem_limit_bytes=67043328
        ),
    )(place_of, neighbor_table.T, owner_map, right_side, coarse_op)


def solution(mesh):
    placed = (P(("grp", "sub"), None, None), P(("grp", "sub"), None, None), P(), P())
    return jax.shard_map(
        per_device,
        mesh=mesh,
        in_specs=placed,
        out_specs=P(("grp", "sub"), None, None),
        check_vma=False,
    )
```
